32 devices in a mesh: sector: 16 (over z, y, x), block: 2 (over core).
Axes of the slice: x: 2, y: 2, z: 4, core: 2. Of those that a mesh axis runs over, the one named last changes fastest.
Arguments:
- adjoint_prev: float32 [5, 16, 128, 128], P(None, 'block', 'sector'), may hold values from -6 to 6
- adjoint_source: float32 [5, 16, 128, 128], P(None, 'block', 'sector'), may hold values from -6 to 6
- face_matrices: bfloat16 [3, 5, 5, 16, 128, 128], P(None, None, None, 'block', 'sector'), may hold values from -2.5 to 2.5
- inverse_blocks: bfloat16 [5, 5, 16, 128, 128], P(None, None, 'block', 'sector')
- sector_offset: int32 [1], replicated, may hold values from 1 to 15
- donor_cells: int32 [128], P('sector'), may hold values from 0 to 7
- donor_weights: float32 [128], P('sector'), may hold values from 0.1 to 0.9
Outputs:
- adjoint: float32 [5, 16, 128, 128], P(None, 'block', 'sector')
- last_update: float32 [5, 16, 128, 128], P(None, 'block', 'sector')
The draws below stay inside these ranges and needn't reach their ends.
All inputs are finite; a program needn't handle non-finite values.
Results may differ from the reference program's by a relative error of at most 0.0003.
Values sent between devices are 32-bit elements; how exact they have to be, the bound alone decides.
A program may use at most 64 MiB of HBM per device.

```python
import jax
import jax.numpy as jnp

CT = 8
NRAD = 128
ITERS = 4
NAX = 16
NCIRC = 128
N_SECTOR = 16


def draw_inverse_blocks(key, part):
    key_off = jax.random.fold_in(key, 11)
    key_diag = jax.random.fold_in(key, 12)
    off_part = 0.06 * jax.random.normal(key_off, (5, 5, NAX, NCIRC, NRAD), jnp.float32)
    diag_part = jnp.exp(jax.random.uniform(key_diag, (5, NAX, NCIRC, NRAD), jnp.float32, jnp.log(0.15), jnp.log(0.3)))
    identity = jnp.eye(5, dtype=jnp.float32)[:, :, None, None, None]
    return (off_part * (1.0 - identity) + identity * diag_part[:, None]).astype(jnp.bfloat16)


def touch_ends(values, key, least, largest):
    longest = values.shape.index(max(values.shape))
    spots = []
    for shift in (0, 1):
        where = [jax.random.randint(jax.random.fold_in(key, axis), (), 0, length) for axis, length in enumerate(values.shape)]
        where[longest] = (where[longest] + shift) % values.shape[longest]
        spots.append(tuple(where))
    return values.at[spots[0]].set(least).at[spots[1]].set(largest)


def block_scale(rng, shape, pieces, low, largest):
    loudness = 1.0
    for dim, blocks in pieces:
        steps = jax.random.uniform(jax.random.fold_in(jax.random.fold_in(rng, 6), dim), (blocks,), jnp.float32, low / len(pieces), largest / len(pieces))
        loudness = loudness * jnp.repeat(jnp.exp(steps), shape[dim] // blocks).reshape((-1,) + (1,) * (len(shape) - 1 - dim))
    return loudness


def scatter_about(key, extent, deviation, reach, shards=(), kind=jnp.bfloat16):
    factor_of = block_scale(key, extent, shards, -0.22, 0.18) if shards else 1.0
    array = jax.random.normal(key, extent, jnp.float32) * deviation * factor_of
    return jnp.minimum(jnp.maximum(array, -reach), reach).astype(kind)


def setup_inputs(seed: int = 0) -> dict:
    streams_of = jax.random.split(jax.random.key(seed), 8)
    return {
        "adjoint_prev": scatter_about(streams_of[0], (5, NAX, NCIRC, NRAD), 1.0, 6.0, ((1, 2), (2, 16)), jnp.float32),
        "adjoint_source": scatter_about(streams_of[1], (5, NAX, NCIRC, NRAD), 1.0, 6.0, ((1, 2), (2, 16)), jnp.float32),
        "face_matrices": scatter_about(streams_of[2], (3, 5, 5, NAX, NCIRC, NRAD), 5 ** -0.5, 2.5, ((3, 2), (4, 16))),
        "inverse_blocks": draw_inverse_blocks(jax.random.fold_in(streams_of[7], 71), 0),
        "sector_offset": jax.random.randint(streams_of[4], (1,), 1, N_SECTOR).astype(jnp.int32),
        "donor_cells": touch_ends(jax.random.randint(streams_of[5], (NCIRC,), 0, CT), jax.random.fold_in(streams_of[5], 1), 0, CT - 1).astype(jnp.int32),
        "donor_weights": jnp.clip(0.1 + 0.79999997 * jax.random.uniform(streams_of[6], (NCIRC,), jnp.float32) ** block_scale(streams_of[6], (NCIRC,), ((0, 16),), -0.2, 0.2), 0.1, 0.9),
    }


def neighbour_terms(adjoint, sector_offset, donor_cells, donor_weights):
    first = NAX // 2
    rotor_row = adjoint[:, first - 1]
    shift_cells = sector_offset[0] * CT
    base = (jnp.arange(NCIRC, dtype=jnp.int32) // CT) * CT + donor_cells
    source_one = jnp.mod(base - shift_cells, NCIRC).astype(jnp.int32)
    source_two = jnp.mod(base + 1 - shift_cells, NCIRC).astype(jnp.int32)
    weights = donor_weights[None, :, None]
    facing = weights * jnp.take(rotor_row, source_one, axis=1) + (1.0 - weights) * jnp.take(rotor_row, source_two, axis=1)
    zero_layer = jnp.zeros_like(adjoint[:, :1])
    axial_minus = jnp.concatenate([zero_layer, adjoint[:, :-1]], axis=1)
    axial_minus = axial_minus.at[:, first].set(facing)
    axial_plus = jnp.concatenate([adjoint[:, 1:], zero_layer], axis=1)
    around_minus = jnp.roll(adjoint, 1, axis=2)
    around_plus = jnp.roll(adjoint, -1, axis=2)
    padded = jnp.pad(adjoint, ((0, 0), (0, 0), (0, 0), (1, 1)))
    radial_minus = padded[:, :, :, :-2]
    radial_plus = padded[:, :, :, 2:]
    return (0.6 * axial_minus + 0.4 * axial_plus,
            0.6 * around_minus + 0.4 * around_plus,
            0.6 * radial_minus + 0.4 * radial_plus)


def sweep(adjoint, adjoint_source, face_matrices, inverse_blocks, sector_offset, donor_cells, donor_weights):
    mixed = neighbour_terms(adjoint, sector_offset, donor_cells, donor_weights)
    coupled = jnp.zeros_like(adjoint)
    for direction in range(3):
        for comp in range(5):
            coupled = coupled + face_matrices[direction, comp].astype(jnp.float32) * mixed[direction][comp][None]
    total = adjoint_source + coupled
    result = jnp.zeros_like(adjoint)
    for comp in range(5):
        result = result + inverse_blocks[:, comp].astype(jnp.float32) * total[comp][None]
    return result


def reference(adjoint_prev, adjoint_source, face_matrices, inverse_blocks, sector_offset, donor_cells, donor_weights):
    adjoint = adjoint_prev
    last_update = jnp.zeros_like(adjoint_prev)
    for sweep_number in range(ITERS):
        result = sweep(adjoint, adjoint_source, face_matrices, inverse_blocks, sector_offset, donor_cells, donor_weights)
        last_update = result - adjoint
        adjoint = result
    return adjoint, last_update
```

```python
import functools

import jax
import jax.numpy as jnp
from jax import lax
from jax.experimental import pallas as pl
from jax.experimental.pallas import tpu as pltpu
from jax.sharding import PartitionSpec as P

ITERS = 4
MESH = pl.DeviceIdType.MESH


def low_part(sectors):
    return max(d for d in range(1, sectors + 1) if sectors % d == 0 and d * d <= sectors)


def kernel(
    sectors,
    blocks,
    prev_ref,
    source_ref,
    face_ref,
    inverse_ref,
    offset_ref,
    cells_ref,
    weights_ref,
    adjoint_ref,
    update_ref,
    field,
    source,
    face16,
    inverse16,
    face,
    inverse,
    partial,
    edge,
    halo,
    rows,
    forward,
    picked,
    blend,
    local_sem,
    edge_send,
    edge_recv,
    rim_send,
    rim_recv,
    row_send,
    row_recv,
    forward_send,
    forward_recv,
):
    comps, layers, around, lanes = prev_ref.shape
    sector = lax.axis_index("sector")
    block = lax.axis_index("block")
    first = blocks // 2
    lows = low_part(sectors)
    highs = sectors // lows
    high, low = sector // lows, sector % lows
    after, before = (sector + 1) % sectors, (sector + sectors - 1) % sectors
    is_stator_face = block == first
    is_rotor_face = block == first - 1

    barrier = pltpu.get_barrier_semaphore()

    def greet(to_sector, to_block):
        pl.semaphore_signal(barrier, inc=1, device_id=(to_sector, to_block), device_id_type=MESH)

    greet(after, block)
    greet(before, block)

    @pl.when(block > 0)
    def _():
        greet(sector, block - 1)

    @pl.when(block < blocks - 1)
    def _():
        greet(sector, block + 1)

    @pl.when(is_rotor_face)
    def _():
        for step in range(highs):
            greet(((high + step) % highs) * lows + low, first)

    @pl.when(is_stator_face)
    def _():
        for step in range(highs):
            greet(((high + step) % highs) * lows + low, first - 1)
        for step in range(1, lows):
            greet(high * lows + (low + step) % lows, first)

    into_field = pltpu.make_async_copy(prev_ref, field.at[0, :, pl.ds(1, layers)], local_sem.at[0])
    into_source = pltpu.make_async_copy(source_ref, source, local_sem.at[1])
    into_face = pltpu.make_async_copy(face_ref, face16, local_sem.at[2])
    into_inverse = pltpu.make_async_copy(inverse_ref, inverse16, local_sem.at[3])
    for copy in (into_field, into_source, into_face, into_inverse):
        copy.start()

    @pl.when(block == 0)
    def _():
        for k in range(ITERS):
            for n in range(comps):
                field[k, n, 0] = jnp.zeros((around, lanes), jnp.float32)

    @pl.when(block == blocks - 1)
    def _():
        for k in range(ITERS):
            for n in range(comps):
                field[k, n, layers + 1] = jnp.zeros((around, lanes), jnp.float32)

    column = lax.broadcasted_iota(jnp.int32, (around, lanes), 0)
    lane = lax.broadcasted_iota(jnp.int32, (around, lanes), 1)
    donor = jnp.zeros((around, lanes), jnp.int32)
    weight = jnp.zeros((around, lanes), jnp.float32)
    for j in range(around):
        donor = jnp.where(column == j, cells_ref[j], donor)
        weight = jnp.where(column == j, weights_ref[j], weight)
    for k in range(around + 1):
        blend[k] = jnp.where(donor == k, weight, 0.0) + jnp.where(donor + 1 == k, 1.0 - weight, 0.0)
    radial_lower = jnp.where(lane == 0, 0.0, 0.6).astype(jnp.float32)
    radial_upper = jnp.where(lane == lanes - 1, 0.0, 0.4).astype(jnp.float32)

    into_field.wait()
    for n in range(comps):
        edge[0, 0, n] = field[0, n, pl.ds(1, layers), around - 1, :]
        edge[0, 1, n] = field[0, n, pl.ds(1, layers), 0, :]

    def edge_copy(k, side):
        return pltpu.make_async_remote_copy(
            src_ref=edge.at[k, side],
            dst_ref=halo.at[k, side],
            send_sem=edge_send.at[k, side],
            recv_sem=edge_recv.at[k, side],
            device_id=(before if side else after, block),
            device_id_type=MESH,
        )

    def rim_copy(k, side):
        return pltpu.make_async_remote_copy(
            src_ref=field.at[k, :, 1 if side else layers],
            dst_ref=field.at[k, :, layers + 1 if side else 0],
            send_sem=rim_send.at[k, side],
            recv_sem=rim_recv.at[k, side],
            device_id=(sector, block - 1 if side else block + 1),
            device_id_type=MESH,
        )

    def row_copy(k, step):
        to = (high + step) % highs
        return pltpu.make_async_remote_copy(
            src_ref=field.at[k, :, layers],
            dst_ref=rows[k].at[high],
            send_sem=row_send.at[k, step],
            recv_sem=row_recv.at[k, step],
            device_id=(to * lows + low, first),
            device_id_type=MESH,
        )

    def row_arrival(k, step):
        origin = (high + highs - step) % highs
        return pltpu.make_async_remote_copy(
            src_ref=field.at[k, :, layers],
            dst_ref=rows[k].at[origin],
            send_sem=row_send.at[k, step],
            recv_sem=row_recv.at[k, step],
            device_id=(origin * lows + low, first),
            device_id_type=MESH,
        )

    def forward_copy(k, step):
        return pltpu.make_async_remote_copy(
            src_ref=forward.at[k],
            dst_ref=picked[k].at[low],
            send_sem=forward_send.at[k, step],
            recv_sem=forward_recv.at[k, step],
            device_id=(high * lows + (low + step) % lows, first),
            device_id_type=MESH,
        )

    def forward_arrival(k, step):
        origin = (low + lows - step) % lows
        return pltpu.make_async_remote_copy(
            src_ref=forward.at[k],
            dst_ref=picked[k].at[origin],
            send_sem=forward_send.at[k, step],
            recv_sem=forward_recv.at[k, step],
            device_id=(high * lows + origin, first),
            device_id_type=MESH,
        )

    def send_rows(k):
        @pl.when(is_rotor_face)
        def _():
            for step in reversed(range(highs)):
                row_copy(k, step).start()

    def send_rims(k):
        @pl.when(block > 0)
        def _():
            rim_copy(k, 1).start()

        @pl.when((block < blocks - 1) & (block != first - 1))
        def _():
            rim_copy(k, 0).start()

    greetings = 2 + (block > 0).astype(jnp.int32) + (block < blocks - 1).astype(jnp.int32)
    greetings += jnp.where(is_rotor_face, highs, 0) + jnp.where(is_stator_face, highs + lows - 1, 0)
    pl.semaphore_wait(barrier, greetings)

    edge_copy(0, 0).start()
    edge_copy(0, 1).start()
    send_rows(0)
    send_rims(0)

    into_face.wait()

    def widen(i, carry):
        for d in range(3):
            for m in range(comps):
                face[d, i, m] = face16[d, i, m].astype(jnp.float32)
        return carry

    lax.fori_loop(0, comps, widen, 0)
    into_inverse.wait()

    def widen_inverse(i, carry):
        for m in range(comps):
            inverse[i, m] = inverse16[i, m].astype(jnp.float32)
        return carry

    lax.fori_loop(0, comps, widen_inverse, 0)
    into_source.wait()

    def radial(k, a, acc):
        for n in range(comps):
            here = field[k, n, a + 1]
            mix = radial_lower * pltpu.roll(here, 1, 1) + radial_upper * pltpu.roll(here, lanes - 1, 1)
            acc = [acc[m] + face[2, n, m, a] * mix for m in range(comps)]
        return acc

    def axial(k, a, acc):
        for n in range(comps):
            mix = 0.6 * field[k, n, a] + 0.4 * field[k, n, a + 2]
            acc = [acc[m] + face[0, n, m, a] * mix for m in range(comps)]
        return acc

    def circumferential(k, a, acc):
        for n in range(comps):
            here = field[k, n, a + 1]
            minus = jnp.where(column == 0, halo[k, 0, n, pl.ds(a, 1), :], pltpu.roll(here, 1, 0))
            plus = jnp.where(column == around - 1, halo[k, 1, n, pl.ds(a, 1), :], pltpu.roll(here, around - 1, 0))
            mix = 0.6 * minus + 0.4 * plus
            acc = [acc[m] + face[1, n, m, a] * mix for m in range(comps)]
        return acc

    def early(k, a, rim):
        acc = radial(k, a, [source[m, a] for m in range(comps)])
        if not rim:
            acc = axial(k, a, acc)
        for m in range(comps):
            partial[m, a] = acc[m]

    def late(k, a, rim):
        acc = circumferential(k, a, [partial[m, a] for m in range(comps)])
        if rim:
            acc = axial(k, a, acc)
        for m in range(comps):
            fresh = inverse[m, 0, a] * acc[0]
            for n in range(1, comps):
                fresh = fresh + inverse[m, n, a] * acc[n]
            if k < ITERS - 1:
                field[k + 1, m, a + 1] = fresh
                edge[k + 1, 0, m, pl.ds(a, 1), :] = fresh[around - 1 :, :]
                edge[k + 1, 1, m, pl.ds(a, 1), :] = fresh[:1, :]
            else:
                adjoint_ref[m, a] = fresh
                update_ref[m, a] = fresh - field[k, m, a + 1]

    offset = offset_ref[0]
    offset_high, offset_low = offset // lows, offset % lows

    def face_the_rotor(k):
        for step in range(highs):
            row_arrival(k, step).wait_recv()
        whole_from = (high + 2 * highs - offset_high - (low + offset_low) // lows) % highs
        first_from = (high + 2 * highs + 1 - offset_high - (low + offset_low + lows - 1) // lows) % highs
        for n in range(comps):
            forward[k, n] = rows[k][whole_from, n]
            forward[k, comps, n : n + 1, :] = rows[k][first_from, n, 0:1, :]
        for step in range(1, lows):
            forward_copy(k, step).start()
        for n in range(comps + 1):
            picked[k][low, n] = forward[k, n]
        for step in range(1, lows):
            forward_arrival(k, step).wait_recv()
        row_of = (low + lows - offset_low) % lows
        next_of = (low + lows - offset_low + 1) % lows
        for n in range(comps):
            total = blend[around] * picked[k][next_of, comps, n : n + 1, :]
            for c in range(around):
                total = total + blend[c] * picked[k][row_of, n, c : c + 1, :]
            field[k, n, 0] = total

    def body_of(step, k, rim):
        def body(a, carry):
            step(k, a, rim)
            return carry

        return body

    for k in range(ITERS):
        lax.fori_loop(1, layers - 1, body_of(early, k, False), 0)
        early(k, 0, True)
        early(k, layers - 1, True)
        edge_copy(k, 0).wait_recv()
        edge_copy(k, 1).wait_recv()
        lax.fori_loop(1, layers - 1, body_of(late, k, False), 0)

        @pl.when(block < blocks - 1)
        def _():
            rim_copy(k, 1).wait_recv()

        @pl.when((block > 0) & (block != first))
        def _():
            rim_copy(k, 0).wait_recv()

        @pl.when(is_stator_face)
        def _():
            face_the_rotor(k)

        late(k, layers - 1, True)
        late(k, 0, True)
        if k < ITERS - 1:
            edge_copy(k + 1, 0).start()
            edge_copy(k + 1, 1).start()
            send_rows(k + 1)
            send_rims(k + 1)

    for k in range(ITERS):
        edge_copy(k, 0).wait_send()
        edge_copy(k, 1).wait_send()

        @pl.when(block > 0)
        def _():
            rim_copy(k, 1).wait_send()

        @pl.when((block < blocks - 1) & (block != first - 1))
        def _():
            rim_copy(k, 0).wait_send()

        @pl.when(is_rotor_face)
        def _():
            for step in range(highs):
                row_copy(k, step).wait_send()

        @pl.when(is_stator_face)
        def _():
            for step in range(1, lows):
                forward_copy(k, step).wait_send()


def solution(mesh):
    sectors, blocks = mesh.shape["sector"], mesh.shape["block"]
    lows = low_part(sectors)
    highs = sectors // lows

    def sweeps(prev, source, face, inverse, offset, cells, weights):
        comps, layers, around, lanes = prev.shape
        f32, dma = jnp.float32, pltpu.SemaphoreType.DMA
        plane = (around, lanes)
        hbm = pl.BlockSpec(memory_space=pl.ANY)
        smem = pl.BlockSpec(memory_space=pltpu.SMEM)
        vmem = pl.BlockSpec(memory_space=pltpu.VMEM)
        return pl.pallas_call(
            functools.partial(kernel, sectors, blocks),
            out_shape=(pltpu.VMEM(prev.shape, f32),) * 2,
            in_specs=[hbm] * 4 + [smem] * 3,
            out_specs=(vmem, vmem),
            scratch_shapes=[
                pltpu.VMEM((ITERS, comps, layers + 2) + plane, f32),
                pltpu.VMEM(prev.shape, f32),
                pltpu.VMEM(face.shape, face.dtype),
                pltpu.VMEM(inverse.shape, inverse.dtype),
                pltpu.VMEM(face.shape, f32),
                pltpu.VMEM(inverse.shape, f32),
                pltpu.VMEM(prev.shape, f32),
                pltpu.VMEM((ITERS, 2, comps, layers, lanes), f32),
                pltpu.VMEM((ITERS, 2, comps, layers, lanes), f32),
                [pltpu.VMEM((highs, comps) + plane, f32)] * ITERS,
                pltpu.VMEM((ITERS, comps + 1) + plane, f32),
                [pltpu.VMEM((lows, comps + 1) + plane, f32)] * ITERS,
                pltpu.VMEM((around + 1,) + plane, f32),
                dma((4,)),
                dma((ITERS, 2)),
                dma((ITERS, 2)),
                dma((ITERS, 2)),
                dma((ITERS, 2)),
                dma((ITERS, highs)),
                dma((ITERS, highs)),
                dma((ITERS, lows)),
                dma((ITERS, lows)),
            ],
            compiler_params=pltpu.CompilerParams(collective_id=0, has_side_effects=True),
        )(prev, source, face, inverse, offset, cells, weights)

    return jax.shard_map(
        sweeps,
        mesh=mesh,
        in_specs=(
            P(None, "block", "sector", None),
            P(None, "block", "sector", None),
            P(None, None, None, "block", "sector", None),
            P(None, None, "block", "sector", None),
            P(),
            P("sector"),
            P("sector"),
        ),
        out_specs=(P(None, "block", "sector", None), P(None, "block", "sector", None)),
        check_vma=False,
    )
```

```python
import functools

import jax
import jax.numpy as jnp
from jax import lax
from jax.experimental import pallas as pl
from jax.experimental.pallas import tpu as pltpu
from jax.sharding import PartitionSpec as P

ITERS = 4
MESH = pl.DeviceIdType.MESH


def low_part(sectors):
    return max(d for d in range(1, sectors + 1) if sectors % d == 0 and d * d <= sectors)


def kernel(
    sectors,
    blocks,
    prev_ref,
    source_ref,
    face_ref,
    inverse_ref,
    offset_hbm,
    cells_hbm,
    weights_hbm,
    adjoint_ref,
    update_ref,
    offset_ref,
    cells_ref,
    weights_ref,
    field,
    source,
    face16,
    inverse16,
    face,
    inverse,
    partial,
    edge,
    halo,
    rows,
    forward,
    picked,
    blend,
    face_edge,
    inverse_edge,
    source_edge,
    partial_edge,
    local_sem,
    edge_send,
    edge_recv,
    rim_send,
    rim_recv,
    row_send,
    row_recv,
    forward_send,
    forward_recv,
):
    comps, layers, around, lanes = prev_ref.shape
    sector = lax.axis_index("sector")
    block = lax.axis_index("block")
    first = blocks // 2
    lows = low_part(sectors)
    highs = sectors // lows
    high, low = sector // lows, sector % lows
    after, before = (sector + 1) % sectors, (sector + sectors - 1) % sectors
    is_stator_face = block == first
    is_rotor_face = block == first - 1

    barrier = pltpu.get_barrier_semaphore()

    def greet(to_sector, to_block):
        pl.semaphore_signal(barrier, inc=1, device_id=(to_sector, to_block), device_id_type=MESH)

    greet(after, block)
    greet(before, block)

    @pl.when(block > 0)
    def _():
        greet(sector, block - 1)

    @pl.when(block < blocks - 1)
    def _():
        greet(sector, block + 1)

    @pl.when(is_rotor_face)
    def _():
        for step in range(highs):
            greet(((high + step) % highs) * lows + low, first)

    @pl.when(is_stator_face)
    def _():
        for step in range(highs):
            greet(((high + step) % highs) * lows + low, first - 1)
        for step in range(1, lows):
            greet(high * lows + (low + step) % lows, first)

    into_field = pltpu.make_async_copy(prev_ref, field.at[0, :, pl.ds(1, layers)], local_sem.at[0])
    into_source = pltpu.make_async_copy(source_ref, source, local_sem.at[1])
    into_face = pltpu.make_async_copy(face_ref, face16, local_sem.at[2])
    into_inverse = pltpu.make_async_copy(inverse_ref, inverse16, local_sem.at[3])
    into_offset = pltpu.make_async_copy(offset_hbm, offset_ref, local_sem.at[4])
    into_cells = pltpu.make_async_copy(cells_hbm, cells_ref, local_sem.at[5])
    into_weights = pltpu.make_async_copy(weights_hbm, weights_ref, local_sem.at[6])
    scalars = (into_offset, into_cells, into_weights)
    for copy in (into_field,) + scalars + (into_face, into_inverse, into_source):
        copy.start()

    @pl.when(block == 0)
    def _():
        for k in range(ITERS):
            for n in range(comps):
                field[k, n, 0] = jnp.zeros((around, lanes), jnp.float32)

    @pl.when(block == blocks - 1)
    def _():
        for k in range(ITERS):
            for n in range(comps):
                field[k, n, layers + 1] = jnp.zeros((around, lanes), jnp.float32)

    for copy in scalars:
        copy.wait()
    column = lax.broadcasted_iota(jnp.int32, (around, lanes), 0)
    lane = lax.broadcasted_iota(jnp.int32, (around, lanes), 1)
    donor = jnp.zeros((around, lanes), jnp.int32)
    weight = jnp.zeros((around, lanes), jnp.float32)
    for j in range(around):
        donor = jnp.where(column == j, cells_ref[j], donor)
        weight = jnp.where(column == j, weights_ref[j], weight)
    for k in range(around + 1):
        blend[k] = jnp.where(donor == k, weight, 0.0) + jnp.where(donor + 1 == k, 1.0 - weight, 0.0)
    radial_lower = jnp.where(lane == 0, 0.0, 0.6).astype(jnp.float32)
    radial_upper = jnp.where(lane == lanes - 1, 0.0, 0.4).astype(jnp.float32)

    into_field.wait()
    for n in range(comps):
        edge[0, 0, n] = field[0, n, pl.ds(1, layers), around - 1, :]
        edge[0, 1, n] = field[0, n, pl.ds(1, layers), 0, :]

    def edge_copy(k, side):
        return pltpu.make_async_remote_copy(
            src_ref=edge.at[k, side],
            dst_ref=halo.at[k, side],
            send_sem=edge_send.at[k, side],
            recv_sem=edge_recv.at[k, side],
            device_id=(before if side else after, block),
            device_id_type=MESH,
        )

    def rim_copy(k, side):
        return pltpu.make_async_remote_copy(
            src_ref=field.at[k, :, 1 if side else layers],
            dst_ref=field.at[k, :, layers + 1 if side else 0],
            send_sem=rim_send.at[k, side],
            recv_sem=rim_recv.at[k, side],
            device_id=(sector, block - 1 if side else block + 1),
            device_id_type=MESH,
        )

    def row_copy(k, step):
        to = (high + step) % highs
        return pltpu.make_async_remote_copy(
            src_ref=field.at[k, :, layers],
            dst_ref=rows[k].at[high],
            send_sem=row_send.at[k, step],
            recv_sem=row_recv.at[k, step],
            device_id=(to * lows + low, first),
            device_id_type=MESH,
        )

    def row_arrival(k, step):
        origin = (high + highs - step) % highs
        return pltpu.make_async_remote_copy(
            src_ref=field.at[k, :, layers],
            dst_ref=rows[k].at[origin],
            send_sem=row_send.at[k, step],
            recv_sem=row_recv.at[k, step],
            device_id=(origin * lows + low, first),
            device_id_type=MESH,
        )

    def forward_copy(k, step):
        return pltpu.make_async_remote_copy(
            src_ref=forward.at[k],
            dst_ref=picked[k].at[low],
            send_sem=forward_send.at[k, step],
            recv_sem=forward_recv.at[k, step],
            device_id=(high * lows + (low + step) % lows, first),
            device_id_type=MESH,
        )

    def forward_arrival(k, step):
        origin = (low + lows - step) % lows
        return pltpu.make_async_remote_copy(
            src_ref=forward.at[k],
            dst_ref=picked[k].at[origin],
            send_sem=forward_send.at[k, step],
            recv_sem=forward_recv.at[k, step],
            device_id=(high * lows + origin, first),
            device_id_type=MESH,
        )

    def send_rows(k):
        @pl.when(is_rotor_face)
        def _():
            for step in reversed(range(highs)):
                row_copy(k, step).start()

    def send_rims(k):
        @pl.when(block > 0)
        def _():
            rim_copy(k, 1).start()

        @pl.when((block < blocks - 1) & (block != first - 1))
        def _():
            rim_copy(k, 0).start()

    greetings = 2 + (block > 0).astype(jnp.int32) + (block < blocks - 1).astype(jnp.int32)
    greetings += jnp.where(is_rotor_face, highs, 0) + jnp.where(is_stator_face, highs + lows - 1, 0)
    pl.semaphore_wait(barrier, greetings)

    edge_copy(0, 0).start()
    edge_copy(0, 1).start()
    send_rows(0)
    send_rims(0)

    into_face.wait()
    rims = (around - 1, 0)

    def widen(i, carry):
        for d in range(3):
            for m in range(comps):
                face[d, i, m] = face16[d, i, m].astype(jnp.float32)
                for side in range(2):
                    face_edge[d, side, i, m] = face[d, i, m, :, rims[side], :]
        return carry

    lax.fori_loop(0, comps, widen, 0)
    into_inverse.wait()

    def widen_inverse(i, carry):
        for m in range(comps):
            inverse[i, m] = inverse16[i, m].astype(jnp.float32)
            for side in range(2):
                inverse_edge[side, i, m] = inverse[i, m, :, rims[side], :]
        return carry

    lax.fori_loop(0, comps, widen_inverse, 0)
    into_source.wait()
    for side in range(2):
        for m in range(comps):
            source_edge[side, m] = source[m, :, rims[side], :]

    edge_lane = lax.broadcasted_iota(jnp.int32, (layers, lanes), 1)
    edge_lower = jnp.where(edge_lane == 0, 0.0, 0.6).astype(jnp.float32)
    edge_upper = jnp.where(edge_lane == lanes - 1, 0.0, 0.4).astype(jnp.float32)

    def early_edge(k, side):
        inner, share = (around - 2, 0.6) if side == 0 else (1, 0.4)
        acc = [source_edge[side, m] for m in range(comps)]
        for n in range(comps):
            own = edge[k, side, n]
            mix = edge_lower * pltpu.roll(own, 1, 1) + edge_upper * pltpu.roll(own, lanes - 1, 1)
            beside = share * field[k, n, pl.ds(1, layers), inner, :]
            for m in range(comps):
                acc[m] = acc[m] + face_edge[2, side, n, m] * mix + face_edge[1, side, n, m] * beside
        for m in range(comps):
            partial_edge[side, m] = acc[m]

    def late_edge(k, side):
        share = 0.4 if side == 0 else 0.6
        acc = [partial_edge[side, m] for m in range(comps)]
        for n in range(comps):
            lower = field[k, n, pl.ds(0, layers), rims[side], :]
            upper = field[k, n, pl.ds(2, layers), rims[side], :]
            mix = 0.6 * lower + 0.4 * upper
            beside = share * halo[k, 1 - side, n]
            for m in range(comps):
                acc[m] = acc[m] + face_edge[0, side, n, m] * mix + face_edge[1, side, n, m] * beside
        for m in range(comps):
            fresh = inverse_edge[side, m, 0] * acc[0]
            for n in range(1, comps):
                fresh = fresh + inverse_edge[side, m, n] * acc[n]
            edge[k + 1, side, m] = fresh

    def radial(k, a, acc):
        for n in range(comps):
            here = field[k, n, a + 1]
            mix = radial_lower * pltpu.roll(here, 1, 1) + radial_upper * pltpu.roll(here, lanes - 1, 1)
            acc = [acc[m] + face[2, n, m, a] * mix for m in range(comps)]
        return acc

    def axial(k, a, acc):
        for n in range(comps):
            mix = 0.6 * field[k, n, a] + 0.4 * field[k, n, a + 2]
            acc = [acc[m] + face[0, n, m, a] * mix for m in range(comps)]
        return acc

    def circumferential(k, a, acc):
        for n in range(comps):
            here = field[k, n, a + 1]
            minus = jnp.where(column == 0, halo[k, 0, n, pl.ds(a, 1), :], pltpu.roll(here, 1, 0))
            plus = jnp.where(column == around - 1, halo[k, 1, n, pl.ds(a, 1), :], pltpu.roll(here, around - 1, 0))
            mix = 0.6 * minus + 0.4 * plus
            acc = [acc[m] + face[1, n, m, a] * mix for m in range(comps)]
        return acc

    def early(k, a, rim):
        acc = radial(k, a, [source[m, a] for m in range(comps)])
        if not rim:
            acc = axial(k, a, acc)
        for m in range(comps):
            partial[m, a] = acc[m]

    def middle(k, a):
        acc = circumferential(k, a, [partial[m, a] for m in range(comps)])
        for m in range(comps):
            partial[m, a] = acc[m]

    def finish(k, a):
        store(k, a, axial(k, a, [partial[m, a] for m in range(comps)]))

    def late(k, a, rim):
        acc = circumferential(k, a, [partial[m, a] for m in range(comps)])
        if rim:
            acc = axial(k, a, acc)
        store(k, a, acc)

    def store(k, a, acc):
        for m in range(comps):
            fresh = inverse[m, 0, a] * acc[0]
            for n in range(1, comps):
                fresh = fresh + inverse[m, n, a] * acc[n]
            if k < ITERS - 1:
                field[k + 1, m, a + 1] = fresh
            else:
                adjoint_ref[m, a] = fresh
                update_ref[m, a] = fresh - field[k, m, a + 1]

    offset = offset_ref[0]
    offset_high, offset_low = offset // lows, offset % lows

    def pass_rows_on(k):
        for step in range(highs):
            row_arrival(k, step).wait_recv()
        whole_from = (high + 2 * highs - offset_high - (low + offset_low) // lows) % highs
        first_from = (high + 2 * highs + 1 - offset_high - (low + offset_low + lows - 1) // lows) % highs
        for n in range(comps):
            forward[k, n] = rows[k][whole_from, n]
            forward[k, comps, n : n + 1, :] = rows[k][first_from, n, 0:1, :]
        for step in range(1, lows):
            forward_copy(k, step).start()
        for n in range(comps + 1):
            picked[k][low, n] = forward[k, n]

    def face_the_rotor(k):
        for step in range(1, lows):
            forward_arrival(k, step).wait_recv()
        row_of = (low + lows - offset_low) % lows
        next_of = (low + lows - offset_low + 1) % lows
        for n in range(comps):
            total = blend[around] * picked[k][next_of, comps, n : n + 1, :]
            for c in range(around):
                total = total + blend[c] * picked[k][row_of, n, c : c + 1, :]
            field[k, n, 0] = total

    def body_of(step, k, rim):
        def body(a, carry):
            step(k, a, rim)
            return carry

        return body

    for k in range(ITERS):
        last = k == ITERS - 1
        lax.fori_loop(1, layers - 1, body_of(early, k, False), 0)
        early(k, 0, True)
        early(k, layers - 1, True)
        if not last:
            early_edge(k, 0)
            early_edge(k, 1)

        @pl.when(is_stator_face)
        def _():
            pass_rows_on(k)

        edge_copy(k, 0).wait_recv()
        edge_copy(k, 1).wait_recv()
        if last:
            lax.fori_loop(1, layers - 1, body_of(late, k, False), 0)
            middle(k, 0)

        @pl.when(block < blocks - 1)
        def _():
            rim_copy(k, 1).wait_recv()

        @pl.when(is_rotor_face)
        def _():
            late(k, layers - 1, True)

        @pl.when((block > 0) & (block != first))
        def _():
            rim_copy(k, 0).wait_recv()

        if last:

            @pl.when(block != first - 1)
            def _():
                late(k, layers - 1, True)

        @pl.when(is_stator_face)
        def _():
            face_the_rotor(k)

        if last:
            finish(k, 0)
        else:
            for side in range(2):
                late_edge(k, side)
                edge_copy(k + 1, side).start()

            @pl.when(is_rotor_face)
            def _():
                for step in reversed(range(highs)):
                    row_copy(k + 1, step).start()

            late(k, 0, True)

            @pl.when(block > 0)
            def _():
                rim_copy(k + 1, 1).start()

            @pl.when(block != first - 1)
            def _():
                late(k, layers - 1, True)

                @pl.when(block < blocks - 1)
                def _():
                    rim_copy(k + 1, 0).start()

            lax.fori_loop(1, layers - 1, body_of(late, k, False), 0)

    for k in range(ITERS):
        edge_copy(k, 0).wait_send()
        edge_copy(k, 1).wait_send()

        @pl.when(block > 0)
        def _():
            rim_copy(k, 1).wait_send()

        @pl.when((block < blocks - 1) & (block != first - 1))
        def _():
            rim_copy(k, 0).wait_send()

        @pl.when(is_rotor_face)
        def _():
            for step in range(highs):
                row_copy(k, step).wait_send()

        @pl.when(is_stator_face)
        def _():
            for step in range(1, lows):
                forward_copy(k, step).wait_send()


def solution(mesh):
    sectors, blocks = mesh.shape["sector"], mesh.shape["block"]
    lows = low_part(sectors)
    highs = sectors // lows

    def sweeps(prev, source, face, inverse, offset, cells, weights):
        comps, layers, around, lanes = prev.shape
        f32, dma = jnp.float32, pltpu.SemaphoreType.DMA
        plane = (around, lanes)
        hbm = pl.BlockSpec(memory_space=pl.ANY)
        vmem = pl.BlockSpec(memory_space=pltpu.VMEM)
        return pl.pallas_call(
            functools.partial(kernel, sectors, blocks),
            out_shape=(pltpu.VMEM(prev.shape, f32),) * 2,
            in_specs=[hbm] * 7,
            out_specs=(vmem, vmem),
            scratch_shapes=[
                pltpu.SMEM(offset.shape, offset.dtype),
                pltpu.SMEM(cells.shape, cells.dtype),
                pltpu.SMEM(weights.shape, weights.dtype),
                pltpu.VMEM((ITERS, comps, layers + 2) + plane, f32),
                pltpu.VMEM(prev.shape, f32),
                pltpu.VMEM(face.shape, face.dtype),
                pltpu.VMEM(inverse.shape, inverse.dtype),
                pltpu.VMEM(face.shape, f32),
                pltpu.VMEM(inverse.shape, f32),
                pltpu.VMEM(prev.shape, f32),
                pltpu.VMEM((ITERS, 2, comps, layers, lanes), f32),
                pltpu.VMEM((ITERS, 2, comps, layers, lanes), f32),
                [pltpu.VMEM((highs, comps) + plane, f32)] * ITERS,
                pltpu.VMEM((ITERS, comps + 1) + plane, f32),
                [pltpu.VMEM((lows, comps + 1) + plane, f32)] * ITERS,
                pltpu.VMEM((around + 1,) + plane, f32),
                pltpu.VMEM((3, 2, comps, comps, layers, lanes), f32),
                pltpu.VMEM((2, comps, comps, layers, lanes), f32),
                pltpu.VMEM((2, comps, layers, lanes), f32),
                pltpu.VMEM((2, comps, layers, lanes), f32),
                dma((7,)),
                dma((ITERS, 2)),
                dma((ITERS, 2)),
                dma((ITERS, 2)),
                dma((ITERS, 2)),
                dma((ITERS, highs)),
                dma((ITERS, highs)),
                dma((ITERS, lows)),
                dma((ITERS, lows)),
            ],
            compiler_params=pltpu.CompilerParams(collective_id=0, has_side_effects=True),
        )(prev, source, face, inverse, offset, cells, weights)

    return jax.shard_map(
        sweeps,
        mesh=mesh,
        in_specs=(
            P(None, "block", "sector", None),
            P(None, "block", "sector", None),
            P(None, None, None, "block", "sector", None),
            P(None, None, "block", "sector", None),
            P(),
            P("sector"),
            P("sector"),
        ),
        out_specs=(P(None, "block", "sector", None), P(None, "block", "sector", None)),
        check_vma=False,
    )
```

```python
import functools

import jax
import jax.numpy as jnp
from jax import lax
from jax.experimental import pallas as pl
from jax.experimental.pallas import tpu as pltpu
from jax.sharding import PartitionSpec as P

ITERS = 4
MESH = pl.DeviceIdType.MESH


def low_part(sectors):
    return max(d for d in range(1, sectors + 1) if sectors % d == 0 and d * d <= sectors)


def kernel(
    sectors,
    blocks,
    prev_ref,
    source_ref,
    face_ref,
    inverse_ref,
    offset_hbm,
    cells_hbm,
    weights_hbm,
    adjoint_ref,
    update_ref,
    offset_ref,
    cells_ref,
    weights_ref,
    field,
    source,
    face16,
    inverse16,
    face,
    inverse,
    partial,
    edge,
    halo,
    rows,
    forward,
    picked,
    blend,
    face_edge,
    inverse_edge,
    source_edge,
    partial_edge,
    local_sem,
    edge_send,
    edge_recv,
    rim_send,
    rim_recv,
    row_send,
    row_recv,
    forward_send,
    forward_recv,
):
    comps, layers, around, lanes = prev_ref.shape
    sector = lax.axis_index("sector")
    block = lax.axis_index("block")
    first = blocks // 2
    lows = low_part(sectors)
    highs = sectors // lows
    high, low = sector // lows, sector % lows
    after, before = (sector + 1) % sectors, (sector + sectors - 1) % sectors
    is_stator_face = block == first
    is_rotor_face = block == first - 1

    barrier = pltpu.get_barrier_semaphore()

    def greet(to_sector, to_block):
        pl.semaphore_signal(barrier, inc=1, device_id=(to_sector, to_block), device_id_type=MESH)

    greet(after, block)
    greet(before, block)

    @pl.when(block > 0)
    def _():
        greet(sector, block - 1)

    @pl.when(block < blocks - 1)
    def _():
        greet(sector, block + 1)

    @pl.when(is_rotor_face)
    def _():
        for step in range(highs):
            greet(((high + step) % highs) * lows + low, first)

    @pl.when(is_stator_face)
    def _():
        for step in range(highs):
            greet(((high + step) % highs) * lows + low, first - 1)
        for step in range(1, lows):
            greet(high * lows + (low + step) % lows, first)

    into_field = pltpu.make_async_copy(prev_ref, field.at[0, :, pl.ds(1, layers)], local_sem.at[0])
    into_source = pltpu.make_async_copy(source_ref, source, local_sem.at[1])
    into_face = pltpu.make_async_copy(face_ref, face16, local_sem.at[2])
    into_inverse = pltpu.make_async_copy(inverse_ref, inverse16, local_sem.at[3])
    into_offset = pltpu.make_async_copy(offset_hbm, offset_ref, local_sem.at[4])
    into_cells = pltpu.make_async_copy(cells_hbm, cells_ref, local_sem.at[5])
    into_weights = pltpu.make_async_copy(weights_hbm, weights_ref, local_sem.at[6])
    scalars = (into_offset, into_cells, into_weights)
    for copy in (into_field,) + scalars + (into_face, into_inverse, into_source):
        copy.start()

    @pl.when(block == 0)
    def _():
        for k in range(ITERS):
            for n in range(comps):
                field[k, n, 0] = jnp.zeros((around, lanes), jnp.float32)

    @pl.when(block == blocks - 1)
    def _():
        for k in range(ITERS):
            for n in range(comps):
                field[k, n, layers + 1] = jnp.zeros((around, lanes), jnp.float32)

    for copy in scalars:
        copy.wait()
    column = lax.broadcasted_iota(jnp.int32, (around, lanes), 0)
    lane = lax.broadcasted_iota(jnp.int32, (around, lanes), 1)
    donor = jnp.zeros((around, lanes), jnp.int32)
    weight = jnp.zeros((around, lanes), jnp.float32)
    for j in range(around):
        donor = jnp.where(column == j, cells_ref[j], donor)
        weight = jnp.where(column == j, weights_ref[j], weight)
    for k in range(around + 1):
        blend[k] = jnp.where(donor == k, weight, 0.0) + jnp.where(donor + 1 == k, 1.0 - weight, 0.0)
    radial_lower = jnp.where(lane == 0, 0.0, 0.6).astype(jnp.float32)
    radial_upper = jnp.where(lane == lanes - 1, 0.0, 0.4).astype(jnp.float32)

    into_field.wait()
    for n in range(comps):
        edge[0, 0, n] = field[0, n, pl.ds(1, layers), around - 1, :]
        edge[0, 1, n] = field[0, n, pl.ds(1, layers), 0, :]

    def edge_copy(k, side):
        return pltpu.make_async_remote_copy(
            src_ref=edge.at[k, side],
            dst_ref=halo.at[k, side],
            send_sem=edge_send.at[k, side],
            recv_sem=edge_recv.at[k, side],
            device_id=(before if side else after, block),
            device_id_type=MESH,
        )

    def rim_copy(k, side):
        return pltpu.make_async_remote_copy(
            src_ref=field.at[k, :, 1 if side else layers],
            dst_ref=field.at[k, :, layers + 1 if side else 0],
            send_sem=rim_send.at[k, side],
            recv_sem=rim_recv.at[k, side],
            device_id=(sector, block - 1 if side else block + 1),
            device_id_type=MESH,
        )

    def row_copy(k, step):
        to = (high + step) % highs
        return pltpu.make_async_remote_copy(
            src_ref=field.at[k, :, layers],
            dst_ref=rows[k].at[high],
            send_sem=row_send.at[k, step],
            recv_sem=row_recv.at[k, step],
            device_id=(to * lows + low, first),
            device_id_type=MESH,
        )

    def row_arrival(k, step):
        origin = (high + highs - step) % highs
        return pltpu.make_async_remote_copy(
            src_ref=field.at[k, :, layers],
            dst_ref=rows[k].at[origin],
            send_sem=row_send.at[k, step],
            recv_sem=row_recv.at[k, step],
            device_id=(origin * lows + low, first),
            device_id_type=MESH,
        )

    def forward_copy(k, step):
        return pltpu.make_async_remote_copy(
            src_ref=forward.at[k],
            dst_ref=picked[k].at[low],
            send_sem=forward_send.at[k, step],
            recv_sem=forward_recv.at[k, step],
            device_id=(high * lows + (low + step) % lows, first),
            device_id_type=MESH,
        )

    def forward_arrival(k, step):
        origin = (low + lows - step) % lows
        return pltpu.make_async_remote_copy(
            src_ref=forward.at[k],
            dst_ref=picked[k].at[origin],
            send_sem=forward_send.at[k, step],
            recv_sem=forward_recv.at[k, step],
            device_id=(high * lows + origin, first),
            device_id_type=MESH,
        )

    def send_rows(k):
        @pl.when(is_rotor_face)
        def _():
            for step in reversed(range(highs)):
                row_copy(k, step).start()

    def send_rims(k):
        @pl.when(block > 0)
        def _():
            rim_copy(k, 1).start()

        @pl.when((block < blocks - 1) & (block != first - 1))
        def _():
            rim_copy(k, 0).start()

    greetings = 2 + (block > 0).astype(jnp.int32) + (block < blocks - 1).astype(jnp.int32)
    greetings += jnp.where(is_rotor_face, highs, 0) + jnp.where(is_stator_face, highs + lows - 1, 0)
    pl.semaphore_wait(barrier, greetings)

    edge_copy(0, 0).start()
    edge_copy(0, 1).start()
    send_rows(0)
    send_rims(0)

    into_face.wait()
    rims = (around - 1, 0)

    def widen(i, carry):
        for d in range(3):
            for m in range(comps):
                face[d, i, m] = face16[d, i, m].astype(jnp.float32)
                for side in range(2):
                    face_edge[d, side, i, m] = face[d, i, m, :, rims[side], :]
        return carry

    lax.fori_loop(0, comps, widen, 0)
    into_inverse.wait()

    def widen_inverse(i, carry):
        for m in range(comps):
            inverse[i, m] = inverse16[i, m].astype(jnp.float32)
            for side in range(2):
                inverse_edge[side, i, m] = inverse[i, m, :, rims[side], :]
        return carry

    lax.fori_loop(0, comps, widen_inverse, 0)
    into_source.wait()
    for side in range(2):
        for m in range(comps):
            source_edge[side, m] = source[m, :, rims[side], :]

    edge_lane = lax.broadcasted_iota(jnp.int32, (layers, lanes), 1)
    edge_lower = jnp.where(edge_lane == 0, 0.0, 0.6).astype(jnp.float32)
    edge_upper = jnp.where(edge_lane == lanes - 1, 0.0, 0.4).astype(jnp.float32)

    def early_edge(k, side):
        inner, share = (around - 2, 0.6) if side == 0 else (1, 0.4)
        acc = [source_edge[side, m] for m in range(comps)]
        for n in range(comps):
            own = edge[k, side, n]
            mix = edge_lower * pltpu.roll(own, 1, 1) + edge_upper * pltpu.roll(own, lanes - 1, 1)
            beside = share * field[k, n, pl.ds(1, layers), inner, :]
            for m in range(comps):
                acc[m] = acc[m] + face_edge[2, side, n, m] * mix + face_edge[1, side, n, m] * beside
        for m in range(comps):
            partial_edge[side, m] = acc[m]

    def late_edge(k, side):
        share = 0.4 if side == 0 else 0.6
        acc = [partial_edge[side, m] for m in range(comps)]
        for n in range(comps):
            lower = field[k, n, pl.ds(0, layers), rims[side], :]
            upper = field[k, n, pl.ds(2, layers), rims[side], :]
            mix = 0.6 * lower + 0.4 * upper
            beside = share * halo[k, 1 - side, n]
            for m in range(comps):
                acc[m] = acc[m] + face_edge[0, side, n, m] * mix + face_edge[1, side, n, m] * beside
        for m in range(comps):
            fresh = inverse_edge[side, m, 0] * acc[0]
            for n in range(1, comps):
                fresh = fresh + inverse_edge[side, m, n] * acc[n]
            edge[k + 1, side, m] = fresh

    def radial(k, a, acc):
        for n in range(comps):
            here = field[k, n, a + 1]
            mix = radial_lower * pltpu.roll(here, 1, 1) + radial_upper * pltpu.roll(here, lanes - 1, 1)
            acc = [acc[m] + face[2, n, m, a] * mix for m in range(comps)]
        return acc

    def axial(k, a, acc):
        for n in range(comps):
            mix = 0.6 * field[k, n, a] + 0.4 * field[k, n, a + 2]
            acc = [acc[m] + face[0, n, m, a] * mix for m in range(comps)]
        return acc

    def circumferential(k, a, acc):
        for n in range(comps):
            here = field[k, n, a + 1]
            minus = jnp.where(column == 0, halo[k, 0, n, pl.ds(a, 1), :], pltpu.roll(here, 1, 0))
            plus = jnp.where(column == around - 1, halo[k, 1, n, pl.ds(a, 1), :], pltpu.roll(here, around - 1, 0))
            mix = 0.6 * minus + 0.4 * plus
            acc = [acc[m] + face[1, n, m, a] * mix for m in range(comps)]
        return acc

    def early(k, a, rim):
        acc = radial(k, a, [source[m, a] for m in range(comps)])
        if not rim:
            acc = axial(k, a, acc)
        for m in range(comps):
            partial[m, a] = acc[m]

    def middle(k, a):
        acc = circumferential(k, a, [partial[m, a] for m in range(comps)])
        for m in range(comps):
            partial[m, a] = acc[m]

    def finish(k, a):
        store(k, a, axial(k, a, [partial[m, a] for m in range(comps)]))

    def late(k, a, rim):
        acc = circumferential(k, a, [partial[m, a] for m in range(comps)])
        if rim:
            acc = axial(k, a, acc)
        store(k, a, acc)

    def store(k, a, acc):
        for m in range(comps):
            fresh = inverse[m, 0, a] * acc[0]
            for n in range(1, comps):
                fresh = fresh + inverse[m, n, a] * acc[n]
            if k < ITERS - 1:
                field[k + 1, m, a + 1] = fresh
            else:
                adjoint_ref[m, a] = 0.0 - fresh
                update_ref[m, a] = field[k, m, a + 1]

    offset = offset_ref[0]
    offset_high, offset_low = offset // lows, offset % lows

    def pass_rows_on(k):
        for step in range(highs):
            row_arrival(k, step).wait_recv()
        whole_from = (high + 2 * highs - offset_high - (low + offset_low) // lows) % highs
        first_from = (high + 2 * highs + 1 - offset_high - (low + offset_low + lows - 1) // lows) % highs
        for n in range(comps):
            forward[k, n] = rows[k][whole_from, n]
            forward[k, comps, n : n + 1, :] = rows[k][first_from, n, 0:1, :]
        for step in range(1, lows):
            forward_copy(k, step).start()
        for n in range(comps + 1):
            picked[k][low, n] = forward[k, n]

    def face_the_rotor(k):
        for step in range(1, lows):
            forward_arrival(k, step).wait_recv()
        row_of = (low + lows - offset_low) % lows
        next_of = (low + lows - offset_low + 1) % lows
        for n in range(comps):
            total = blend[around] * picked[k][next_of, comps, n : n + 1, :]
            for c in range(around):
                total = total + blend[c] * picked[k][row_of, n, c : c + 1, :]
            field[k, n, 0] = total

    def body_of(step, k, rim):
        def body(a, carry):
            step(k, a, rim)
            return carry

        return body

    for k in range(ITERS):
        last = k == ITERS - 1
        lax.fori_loop(1, layers - 1, body_of(early, k, False), 0)
        early(k, 0, True)
        early(k, layers - 1, True)
        if not last:
            early_edge(k, 0)
            early_edge(k, 1)

        @pl.when(is_stator_face)
        def _():
            pass_rows_on(k)

        edge_copy(k, 0).wait_recv()
        edge_copy(k, 1).wait_recv()
        if last:
            lax.fori_loop(1, layers - 1, body_of(late, k, False), 0)
            middle(k, 0)

        @pl.when(block < blocks - 1)
        def _():
            rim_copy(k, 1).wait_recv()

        @pl.when(is_rotor_face)
        def _():
            late(k, layers - 1, True)

        @pl.when((block > 0) & (block != first))
        def _():
            rim_copy(k, 0).wait_recv()

        if last:

            @pl.when(block != first - 1)
            def _():
                late(k, layers - 1, True)

        @pl.when(is_stator_face)
        def _():
            face_the_rotor(k)

        if last:
            finish(k, 0)
        else:
            for side in range(2):
                late_edge(k, side)
                edge_copy(k + 1, side).start()

            @pl.when(is_rotor_face)
            def _():
                for step in reversed(range(highs)):
                    row_copy(k + 1, step).start()

            late(k, 0, True)

            @pl.when(block > 0)
            def _():
                rim_copy(k + 1, 1).start()

            @pl.when(block != first - 1)
            def _():
                late(k, layers - 1, True)

                @pl.when(block < blocks - 1)
                def _():
                    rim_copy(k + 1, 0).start()

            lax.fori_loop(1, layers - 1, body_of(late, k, False), 0)

    for k in range(ITERS):
        edge_copy(k, 0).wait_send()
        edge_copy(k, 1).wait_send()

        @pl.when(block > 0)
        def _():
            rim_copy(k, 1).wait_send()

        @pl.when((block < blocks - 1) & (block != first - 1))
        def _():
            rim_copy(k, 0).wait_send()

        @pl.when(is_rotor_face)
        def _():
            for step in range(highs):
                row_copy(k, step).wait_send()

        @pl.when(is_stator_face)
        def _():
            for step in range(1, lows):
                forward_copy(k, step).wait_send()


def solution(mesh):
    sectors, blocks = mesh.shape["sector"], mesh.shape["block"]
    lows = low_part(sectors)
    highs = sectors // lows

    def sweeps(prev, source, face, inverse, offset, cells, weights):
        comps, layers, around, lanes = prev.shape
        f32, dma = jnp.float32, pltpu.SemaphoreType.DMA
        plane = (around, lanes)
        hbm = pl.BlockSpec(memory_space=pl.ANY)
        vmem = pl.BlockSpec(memory_space=pltpu.VMEM)
        negative, previous = pl.pallas_call(
            functools.partial(kernel, sectors, blocks),
            out_shape=(pltpu.VMEM(prev.shape, f32),) * 2,
            in_specs=[hbm] * 7,
            out_specs=(vmem, vmem),
            scratch_shapes=[
                pltpu.SMEM(offset.shape, offset.dtype),
                pltpu.SMEM(cells.shape, cells.dtype),
                pltpu.SMEM(weights.shape, weights.dtype),
                pltpu.VMEM((ITERS, comps, layers + 2) + plane, f32),
                pltpu.VMEM(prev.shape, f32),
                pltpu.VMEM(face.shape, face.dtype),
                pltpu.VMEM(inverse.shape, inverse.dtype),
                pltpu.VMEM(face.shape, f32),
                pltpu.VMEM(inverse.shape, f32),
                pltpu.VMEM(prev.shape, f32),
                pltpu.VMEM((ITERS, 2, comps, layers, lanes), f32),
                pltpu.VMEM((ITERS, 2, comps, layers, lanes), f32),
                [pltpu.VMEM((highs, comps) + plane, f32)] * ITERS,
                pltpu.VMEM((ITERS, comps + 1) + plane, f32),
                [pltpu.VMEM((lows, comps + 1) + plane, f32)] * ITERS,
                pltpu.VMEM((around + 1,) + plane, f32),
                pltpu.VMEM((3, 2, comps, comps, layers, lanes), f32),
                pltpu.VMEM((2, comps, comps, layers, lanes), f32),
                pltpu.VMEM((2, comps, layers, lanes), f32),
                pltpu.VMEM((2, comps, layers, lanes), f32),
                dma((7,)),
                dma((ITERS, 2)),
                dma((ITERS, 2)),
                dma((ITERS, 2)),
                dma((ITERS, 2)),
                dma((ITERS, highs)),
                dma((ITERS, highs)),
                dma((ITERS, lows)),
                dma((ITERS, lows)),
            ],
            compiler_params=pltpu.CompilerParams(collective_id=0, has_side_effects=True),
        )(prev, source, face, inverse, offset, cells, weights)
        return 0.0 - negative, 0.0 - negative - previous

    return jax.shard_map(
        sweeps,
        mesh=mesh,
        in_specs=(
            P(None, "block", "sector", None),
            P(None, "block", "sector", None),
            P(None, None, None, "block", "sector", None),
            P(None, None, "block", "sector", None),
            P(),
            P("sector"),
            P("sector"),
        ),
        out_specs=(P(None, "block", "sector", None), P(None, "block", "sector", None)),
        check_vma=False,
    )
```
